32 devices in a mesh: slab: 16 (over z, y, x), pencil: 2 (over core).
Axes of the slice: x: 2, y: 2, z: 4, core: 2. Of those that a mesh axis runs over, the one named last changes fastest.
Arguments:
- density: float32 [96, 768, 384], P('slab', 'pencil'), may hold values from 0 to 1
- cell_kind: int32 [96, 768, 384], P('slab', 'pencil'), may hold values from 0 to 2
- sharpness: float32 [1], replicated, may hold values from 48 to 96
- fraction: float32 [1], replicated, may hold values from 0.36 to 0.41
Outputs:
- physical: float32 [96, 768, 384], P('slab', 'pencil')
- threshold: float32 [1], replicated
The draws below stay inside these ranges and needn't reach their ends.
Inputs may be any that keep to these rules, and one draw needn't show every extreme that they name: `cell_kind`: each cell is a design, void or solid cell.
All inputs are finite; a program needn't handle non-finite values.
Results may differ from the reference program's by a relative error of at most 0.0003.
Values sent between devices are 32-bit elements; how exact they have to be, the bound alone decides.
A program may use at most 128 MiB of HBM per device.

```python
import math
import jax
import jax.numpy as jnp
from jax import lax

RADIUS = 5
ITERS = 3
NZ = 96
NY = 768
NX = 384


def draw_density(key, part):
    wave_draw = jax.random.uniform(jax.random.fold_in(key, 11), (6, 3), jnp.float32)
    sign_flip = jnp.where(jax.random.bernoulli(jax.random.fold_in(key, 12), 0.5, (6, 3)), 1.0, -1.0)
    phase_shift = jax.random.uniform(jax.random.fold_in(key, 13), (6,), jnp.float32, -math.pi, math.pi)
    cycles = sign_flip / (24.0 * jnp.power(4.0, wave_draw))
    depth_axis = jnp.arange(NZ, dtype=jnp.float32)[:, None, None]
    row_axis = jnp.arange(NY, dtype=jnp.float32)[None, :, None]
    column_axis = jnp.arange(NX, dtype=jnp.float32)[None, None, :]
    pattern = jnp.zeros((NZ, NY, NX), jnp.float32)
    for component in range(6):
        argument = cycles[component, 0] * depth_axis + cycles[component, 1] * row_axis + cycles[component, 2] * column_axis
        pattern = pattern + jnp.cos(2.0 * math.pi * argument + phase_shift[component])
    pattern = pattern / math.sqrt(3.0)
    middle_value = 0.62
    amplitude = 0.3
    roughness = 0.2
    jitter = jax.random.uniform(jax.random.fold_in(key, 14), (NZ, NY, NX), jnp.float32, -roughness, roughness)
    return jnp.clip(middle_value + amplitude * pattern + jitter, 0.0, 1.0).astype(jnp.float32)


def set_ends(result, stream_key, low, largest):
    dims = result.shape
    place = [jax.random.randint(jax.random.fold_in(stream_key, axis), (), 0, dims[axis]) for axis in range(len(dims))]
    result = result.at[tuple(place)].set(low)
    longest = dims.index(max(dims))
    place[longest] = (place[longest] + 1) % dims[longest]
    return result.at[tuple(place)].set(largest)


def setup_inputs(seed: int = 0) -> dict:
    key_list = jax.random.split(jax.random.key(seed), 5)
    density = draw_density(jax.random.fold_in(key_list[4], 71), 0)
    cell_kind = set_ends(jax.random.randint(key_list[1], (NZ, NY, NX), 0, 3), jax.random.fold_in(key_list[1], 1), 0, 2).astype(jnp.int32)
    sharpness = jnp.clip(jnp.exp(jax.random.uniform(key_list[2], (1,), jnp.float32, math.log(48.0), math.log(96.0))), 48.0, 96.0)
    fraction = jnp.clip(jax.random.uniform(key_list[3], (1,), jnp.float32, 0.36, 0.41), 0.36, 0.41)
    return dict(density=density, cell_kind=cell_kind, sharpness=sharpness, fraction=fraction)


def smooth_axis(field, axis):
    length = field.shape[axis]
    pads = [(0, 0), (0, 0), (0, 0)]
    pads[axis] = (RADIUS, RADIUS)
    padded = jnp.pad(field, pads)
    total = jnp.zeros_like(field)
    for offset in range(-RADIUS, RADIUS + 1):
        weight = float(RADIUS + 1 - abs(offset))
        piece = lax.slice_in_dim(padded, RADIUS + offset, RADIUS + offset + length, axis=axis)
        total = total + weight * piece
    return total


def coverage(count):
    index = jnp.arange(count, dtype=jnp.int32)
    total = jnp.zeros((count,), jnp.float32)
    for offset in range(-RADIUS, RADIUS + 1):
        inside = ((index + offset >= 0) & (index + offset < count)).astype(jnp.float32)
        total = total + float(RADIUS + 1 - abs(offset)) * inside
    return total


def project(filtered, cell_kind, beta, level):
    tangent = jnp.tanh(beta * (filtered - level))
    design = cell_kind == 0
    solid = cell_kind == 2
    values = jnp.where(design, 0.5 * (1.0 + tangent), jnp.where(solid, 1.0, 0.0))
    return values, tangent, design


def reference(density, cell_kind, sharpness, fraction):
    smoothed = smooth_axis(smooth_axis(smooth_axis(density, 0), 1), 2)
    cover = coverage(NZ)[:, None, None] * coverage(NY)[None, :, None] * coverage(NX)[None, None, :]
    filtered = smoothed / cover
    beta = sharpness[0]
    cells = jnp.float32(NZ * NY * NX)
    level = jnp.float32(0.5)
    for step in range(ITERS):
        values, tangent, design = project(filtered, cell_kind, beta, level)
        volume = jnp.sum(values)
        slope = cells + jnp.sum(jnp.where(design, 0.5 * beta * (1.0 - tangent * tangent), 0.0))
        level = level + (volume - fraction[0] * cells) / slope
    values, tangent, design = project(filtered, cell_kind, beta, level)
    return values, jnp.reshape(level, (1,)).astype(jnp.float32)
```

```python
import functools

import jax
import jax.numpy as jnp
from jax import lax
from jax.experimental import pallas as pl
from jax.experimental.pallas import tpu as pltpu
from jax.sharding import PartitionSpec as P

RADIUS = 5
ITERS = 3
CHUNK = 16
PAD = 8
WINDOW = 4
LAG = 2
LANES = 128
FAR = 1.0e6
MESH = pl.DeviceIdType.MESH


def box(values):
    pairs = [a + b for a, b in zip(values[:-1], values[1:])]
    return [pairs[k] + pairs[k + 2] + pairs[k + 4] for k in range(len(values) - RADIUS)]


def triangle(k):
    k = jnp.maximum(k, 0)
    return (k * (k + 1)) // 2


def coverage(index, whole):
    full = (RADIUS + 1) * (RADIUS + 1)
    return (full - triangle(RADIUS - index) - triangle(RADIUS + 1 + index - whole)).astype(jnp.float32)


def split(x):
    high = x.astype(jnp.bfloat16)
    return high, (x - high.astype(jnp.float32)).astype(jnp.bfloat16)


def band(shape, shift):
    row = lax.broadcasted_iota(jnp.int32, shape, 0)
    col = lax.broadcasted_iota(jnp.int32, shape, 1)
    return jnp.maximum(RADIUS + 1 - jnp.abs(col - shift - row), 0).astype(jnp.float32).astype(jnp.bfloat16)


def folded(x):
    tiles = [
        x[i : i + 8, j : j + LANES] for i in range(0, x.shape[0], 8) for j in range(0, x.shape[1], LANES)
    ]
    while len(tiles) > 1:
        tiles = [sum(tiles[i : i + 2][1:], tiles[i]) for i in range(0, len(tiles), 2)]
    return tiles[0]


def kernel(slabs, pencils, beta_ref, fraction_ref, density, kind, coded_out, level_out, own, near, far, kinds,
           along_z, coded, x_band, acc, parts, x_send, x_recv, f_send, f_recv, h_send, h_recv, local_sem,
           r_send, r_recv):
    depth, rows, cols = density.shape
    steps = rows // CHUNK
    slab = lax.axis_index("slab")
    pencil = lax.axis_index("pencil")
    even = slab % 2 == 0
    first = pencil == 0
    devices = slabs * pencils
    me = slab * pencils + pencil

    barrier = pltpu.get_barrier_semaphore()

    @pl.loop(1, devices)
    def _(k):
        other = (me + k) % devices
        pl.semaphore_signal(barrier, inc=1, device_id=(other // pencils, other % pencils), device_id_type=MESH)

    partner = slab + jnp.where(even, 1, -1)
    target = slab + jnp.where(even, 2, -2)
    source = slab - jnp.where(even, 2, -2)
    has_target = (target >= 0) & (target < slabs)
    has_source = (source >= 0) & (source < slabs)
    target = jnp.clip(target, 0, slabs - 1)
    sibling = 1 - pencil
    halo = pl.multiple_of(jnp.where(first, PAD + rows, 0), 8)
    edge = pl.multiple_of(jnp.where(first, 0, PAD + rows), 8)
    there = pl.multiple_of(jnp.where(first, 0, PAD + rows), 8)
    mine = pl.multiple_of(jnp.where(first, rows, PAD), 8)

    def row_of(k):
        return pl.multiple_of(jnp.where(first, steps - 1 - k, k) * CHUNK, CHUNK)

    def x_copy(k):
        r = row_of(k)
        return pltpu.make_async_remote_copy(
            density.at[:, pl.ds(r, CHUNK), :], near.at[:, pl.ds(r + PAD, CHUNK), :],
            x_send.at[k], x_recv.at[k], device_id=(partner, pencil), device_id_type=MESH)

    def f_copy(k):
        r = row_of(k)
        start = jnp.where(even, depth - RADIUS, 0)
        return pltpu.make_async_remote_copy(
            near.at[pl.ds(start, RADIUS), pl.ds(r + PAD, CHUNK), :], far.at[:, pl.ds(r + PAD, CHUNK), :],
            f_send.at[k], f_recv.at[k], device_id=(target, pencil), device_id_type=MESH)

    def halo_copy(index, src, dst):
        return pltpu.make_async_remote_copy(
            src, dst, h_send.at[index], h_recv.at[index], device_id=(slab, sibling), device_id_type=MESH)

    own_row = pl.multiple_of(jnp.where(first, rows - PAD, 0), 8)
    own_halo = halo_copy(0, density.at[:, pl.ds(own_row, PAD), :], own.at[:, pl.ds(there, PAD), :])
    near_halo = halo_copy(1, near.at[:, pl.ds(mine, PAD), :], near.at[:, pl.ds(there, PAD), :])
    far_halo = halo_copy(2, far.at[:, pl.ds(mine, PAD), :], far.at[:, pl.ds(there, PAD), :])
    own_load = pltpu.make_async_copy(density, own.at[:, pl.ds(PAD, rows), :], local_sem.at[0])
    kind_load = pltpu.make_async_copy(kind, kinds, local_sem.at[1])
    coded_store = pltpu.make_async_copy(coded, coded_out, local_sem.at[2])

    pl.semaphore_wait(barrier, devices - 1)
    for k in range(min(WINDOW, steps)):
        x_copy(k).start()
    own_halo.start()
    own_load.start()
    kind_load.start()

    x_band[...] = band((cols, cols), 0)
    acc[...] = jnp.zeros_like(acc)
    along_z[:, pl.ds(edge, PAD), :] = jnp.zeros((depth, PAD, cols), jnp.float32)

    @pl.when(jnp.logical_not(has_source))
    def _():
        @pl.loop(0, RADIUS)
        def _(k):
            far[k] = jnp.zeros(far.shape[1:], jnp.float32)

    beta = beta_ref[0]

    def filter_z(start, count):
        for r in range(0, count, 8):
            for c in range(0, cols, LANES):
                at = (pl.ds(pl.multiple_of(start + r, 8), 8), pl.ds(c, LANES))
                values = [far[jnp.where(even, m, RADIUS - 1 - m), at[0], at[1]] for m in range(RADIUS)]
                values += [own[jnp.where(even, i, depth - 1 - i), at[0], at[1]] for i in range(depth)]
                values += [near[jnp.where(even, i, depth - 1 - i), at[0], at[1]] for i in range(RADIUS)]
                for i, out in enumerate(box(box(values))):
                    along_z[jnp.where(even, i, depth - 1 - i), at[0], at[1]] = out

    def filter_yx(j):
        r = row_of(j)
        y_band = band((CHUNK, CHUNK + 2 * PAD), PAD)
        pieces = []
        for layer in range(depth):
            high, low = split(along_z[layer, pl.ds(r, CHUNK + 2 * PAD), :])
            pieces.append(jnp.dot(y_band, high, preferred_element_type=jnp.float32)
                          + jnp.dot(y_band, low, preferred_element_type=jnp.float32))
        high, low = split(jnp.concatenate(pieces, axis=0))
        smoothed = (jnp.dot(high, x_band[...], preferred_element_type=jnp.float32)
                    + jnp.dot(low, x_band[...], preferred_element_type=jnp.float32))
        row = lax.broadcasted_iota(jnp.int32, (CHUNK, cols), 0) + (pencil * rows + r)
        col = lax.broadcasted_iota(jnp.int32, (CHUNK, cols), 1)
        cover_y = coverage(row, rows * pencils)
        cover_x = coverage(col, cols)
        for layer in range(depth):
            depth_index = jnp.full((1, cols), slab * depth + layer, jnp.int32)
            cover = coverage(depth_index, slabs * depth) * cover_y * cover_x
            filtered = smoothed[layer * CHUNK : (layer + 1) * CHUNK] / cover
            which = kinds[layer, pl.ds(r, CHUNK), :]
            value = jnp.where(which == 0, filtered, jnp.where(which == 2, FAR, -FAR))
            coded[layer, pl.ds(r, CHUNK), :] = value
            tangent = jnp.tanh(beta * (value - 0.5))
            acc[0] += folded(tangent)
            acc[1] += folded(1.0 - tangent * tangent)

    @pl.loop(0, steps + LAG + 1)
    def _(k):
        @pl.when(k < steps)
        def _():
            x_copy(k).wait_recv()

            @pl.when(has_target)
            def _():
                f_copy(k).start()

            @pl.when(k == 0)
            def _():
                near_halo.start()

        @pl.when(k + WINDOW < steps)
        def _():
            x_copy(k + WINDOW).start()

        @pl.when((k >= LAG) & (k < steps + LAG))
        def _():
            @pl.when(has_source)
            def _():
                f_copy(k - LAG).wait_recv()

                @pl.when(k == LAG)
                def _():
                    far_halo.start()

            @pl.when(k == LAG)
            def _():
                own_load.wait()
                kind_load.wait()

            filter_z(row_of(k - LAG) + PAD, CHUNK)

        @pl.when(k == LAG + 1)
        def _():
            own_halo.wait_recv()
            near_halo.wait_recv()

            @pl.when(has_source)
            def _():
                far_halo.wait_recv()

            filter_z(halo, PAD)

        @pl.when(k >= LAG + 1)
        def _():
            filter_yx(k - LAG - 1)

    coded_store.start()

    cells = float(devices) * float(depth * rows * cols)
    level = jnp.full((1, 1), 0.5, jnp.float32)
    for step in range(ITERS):
        if step:
            center = jnp.broadcast_to(level, (8, cols))

            def body(i, carry):
                total, bend = carry
                for layer in range(depth):
                    tangent = jnp.tanh(beta * (coded[layer, pl.ds(pl.multiple_of(i * 8, 8), 8), :] - center))
                    total = total + tangent
                    bend = bend + (1.0 - tangent * tangent)
                return total, bend

            zero = jnp.zeros((8, cols), jnp.float32)
            total, bend = lax.fori_loop(0, rows // 8, body, (zero, zero))
            total, bend = folded(total), folded(bend)
        else:
            total, bend = acc[0], acc[1]
        parts[step, me] = jnp.concatenate(
            [jnp.sum(total, axis=0, keepdims=True), jnp.sum(bend, axis=0, keepdims=True)], axis=0)

        @pl.loop(1, devices)
        def _(k):
            other = (me + k) % devices
            pltpu.make_async_remote_copy(
                parts.at[step, me], parts.at[step, me], r_send.at[step], r_recv.at[step],
                device_id=(other // pencils, other % pencils), device_id_type=MESH).start()

        most = parts.at[step, pl.ds(0, devices - 1)]
        pltpu.make_async_copy(most, most, r_recv.at[step]).wait()
        both = jnp.sum(jnp.sum(parts[step], axis=0), axis=1, keepdims=True)
        volume = 0.5 * (cells + both[0:1])
        slope = cells + 0.5 * beta * both[1:2]
        level = level + (volume - fraction_ref[0] * cells) / slope
    level_out[...] = jnp.broadcast_to(level, level_out.shape)

    @pl.loop(0, steps)
    def _(k):
        x_copy(k).wait_send()

        @pl.when(has_target)
        def _():
            f_copy(k).wait_send()

    own_halo.wait_send()
    near_halo.wait_send()

    @pl.when(has_source)
    def _():
        far_halo.wait_send()

    for step in range(ITERS):
        most = parts.at[step, pl.ds(0, devices - 1)]
        pltpu.make_async_copy(most, most, r_send.at[step]).wait()
    coded_store.wait()


def solution(mesh):
    slabs, pencils = mesh.shape["slab"], mesh.shape["pencil"]

    def local(density, cell_kind, sharpness, fraction):
        depth, rows, cols = density.shape
        steps = rows // CHUNK
        wide = rows + 2 * PAD
        coded, level = pl.pallas_call(
            functools.partial(kernel, slabs, pencils),
            out_shape=(jax.ShapeDtypeStruct(density.shape, jnp.float32), jax.ShapeDtypeStruct((1, LANES), jnp.float32)),
            in_specs=[pl.BlockSpec(memory_space=pltpu.SMEM)] * 2 + [pl.BlockSpec(memory_space=pl.ANY)] * 2,
            out_specs=(pl.BlockSpec(memory_space=pl.ANY), pl.BlockSpec(memory_space=pltpu.VMEM)),
            scratch_shapes=[
                pltpu.VMEM((depth, wide, cols), jnp.float32),
                pltpu.VMEM((depth, wide, cols), jnp.float32),
                pltpu.VMEM((RADIUS, wide, cols), jnp.float32),
                pltpu.VMEM((depth, rows, cols), jnp.int32),
                pltpu.VMEM((depth, wide, cols), jnp.float32),
                pltpu.VMEM((depth, rows, cols), jnp.float32),
                pltpu.VMEM((cols, cols), jnp.bfloat16),
                pltpu.VMEM((2, 8, LANES), jnp.float32),
                pltpu.VMEM((ITERS, slabs * pencils, 2, LANES), jnp.float32),
                pltpu.SemaphoreType.DMA((steps,)),
                pltpu.SemaphoreType.DMA((steps,)),
                pltpu.SemaphoreType.DMA((steps,)),
                pltpu.SemaphoreType.DMA((steps,)),
                pltpu.SemaphoreType.DMA((3,)),
                pltpu.SemaphoreType.DMA((3,)),
                pltpu.SemaphoreType.DMA((3,)),
                pltpu.SemaphoreType.DMA((ITERS,)),
                pltpu.SemaphoreType.DMA((ITERS,)),
            ],
            compiler_params=pltpu.CompilerParams(
                collective_id=0, has_side_effects=True, vmem_limit_bytes=40 * 1024 * 1024),
        )(sharpness, fraction, density, cell_kind)
        threshold = level[0, :1]
        physical = 0.5 * (1.0 + jnp.tanh(sharpness[0] * (coded - threshold[0])))
        return physical, threshold

    in_specs = (P("slab", "pencil", None), P("slab", "pencil", None), P(), P())
    out_specs = (P("slab", "pencil", None), P())
    return jax.shard_map(local, mesh=mesh, in_specs=in_specs, out_specs=out_specs, check_vma=False)
```

```python
import functools

import jax
import jax.numpy as jnp
from jax import lax
from jax.experimental import pallas as pl
from jax.experimental.pallas import tpu as pltpu
from jax.sharding import PartitionSpec as P

RADIUS = 5
ITERS = 3
CHUNK = 16
PAD = 8
WINDOW = 4
LEAD = 8
LANES = 128
FAR = 1.0e6
MESH = pl.DeviceIdType.MESH


def box(values):
    pairs = [a + b for a, b in zip(values[:-1], values[1:])]
    return [pairs[k] + pairs[k + 2] + pairs[k + 4] for k in range(len(values) - RADIUS)]


def triangle(k):
    k = jnp.maximum(k, 0)
    return (k * (k + 1)) // 2


def coverage(index, whole):
    full = (RADIUS + 1) * (RADIUS + 1)
    return (full - triangle(RADIUS - index) - triangle(RADIUS + 1 + index - whole)).astype(jnp.float32)


def split(x):
    high = x.astype(jnp.bfloat16)
    return high, (x - high.astype(jnp.float32)).astype(jnp.bfloat16)


def band(shape, shift):
    row = lax.broadcasted_iota(jnp.int32, shape, 0)
    col = lax.broadcasted_iota(jnp.int32, shape, 1)
    return jnp.maximum(RADIUS + 1 - jnp.abs(col - shift - row), 0).astype(jnp.float32).astype(jnp.bfloat16)


def folded(x):
    tiles = [
        x[i : i + 8, j : j + LANES] for i in range(0, x.shape[0], 8) for j in range(0, x.shape[1], LANES)
    ]
    while len(tiles) > 1:
        tiles = [sum(tiles[i : i + 2][1:], tiles[i]) for i in range(0, len(tiles), 2)]
    return tiles[0]


def kernel(slabs, pencils, beta_ref, fraction_ref, density, kind, coded, level_out, own, near, far, kinds,
           along_z, x_band, acc, parts, x_send, x_recv, b_send, b_recv, f_send, f_recv, h_send, h_recv, local_sem,
           r_send, r_recv):
    depth, rows, cols = density.shape
    steps = rows // CHUNK
    lead = min(LEAD, steps)
    lag = lead + 1
    slab = lax.axis_index("slab")
    pencil = lax.axis_index("pencil")
    even = slab % 2 == 0
    first = pencil == 0
    devices = slabs * pencils
    me = slab * pencils + pencil

    barrier = pltpu.get_barrier_semaphore()

    @pl.loop(1, devices)
    def _(k):
        other = (me + k) % devices
        pl.semaphore_signal(barrier, inc=1, device_id=(other // pencils, other % pencils), device_id_type=MESH)

    partner = slab + jnp.where(even, 1, -1)
    target = slab + jnp.where(even, 2, -2)
    source = slab - jnp.where(even, 2, -2)
    has_target = (target >= 0) & (target < slabs)
    has_source = (source >= 0) & (source < slabs)
    target = jnp.clip(target, 0, slabs - 1)
    sibling = 1 - pencil
    halo = pl.multiple_of(jnp.where(first, PAD + rows, 0), 8)
    edge = pl.multiple_of(jnp.where(first, 0, PAD + rows), 8)
    there = pl.multiple_of(jnp.where(first, 0, PAD + rows), 8)
    mine = pl.multiple_of(jnp.where(first, rows, PAD), 8)

    def row_of(k):
        return pl.multiple_of(jnp.where(first, steps - 1 - k, k) * CHUNK, CHUNK)

    def x_copy(k):
        r = row_of(k)
        layers = pl.ds(jnp.where(even, 0, depth - RADIUS), RADIUS)
        return pltpu.make_async_remote_copy(
            density.at[layers, pl.ds(r, CHUNK), :], near.at[layers, pl.ds(r + PAD, CHUNK), :],
            x_send.at[k], x_recv.at[k], device_id=(partner, pencil), device_id_type=MESH)

    def b_copy(k):
        r = row_of(k)
        layers = pl.ds(jnp.where(even, RADIUS, 0), depth - RADIUS)
        return pltpu.make_async_remote_copy(
            density.at[layers, pl.ds(r, CHUNK), :], near.at[layers, pl.ds(r + PAD, CHUNK), :],
            b_send.at[k], b_recv.at[k], device_id=(partner, pencil), device_id_type=MESH)

    def f_copy(k):
        r = row_of(k)
        start = jnp.where(even, depth - RADIUS, 0)
        return pltpu.make_async_remote_copy(
            near.at[pl.ds(start, RADIUS), pl.ds(r + PAD, CHUNK), :], far.at[:, pl.ds(r + PAD, CHUNK), :],
            f_send.at[k], f_recv.at[k], device_id=(target, pencil), device_id_type=MESH)

    def halo_copy(index, src, dst):
        return pltpu.make_async_remote_copy(
            src, dst, h_send.at[index], h_recv.at[index], device_id=(slab, sibling), device_id_type=MESH)

    own_row = pl.multiple_of(jnp.where(first, rows - PAD, 0), 8)
    own_halo = halo_copy(0, density.at[:, pl.ds(own_row, PAD), :], own.at[:, pl.ds(there, PAD), :])
    near_halo = halo_copy(1, near.at[:, pl.ds(mine, PAD), :], near.at[:, pl.ds(there, PAD), :])
    far_halo = halo_copy(2, far.at[:, pl.ds(mine, PAD), :], far.at[:, pl.ds(there, PAD), :])
    own_load = pltpu.make_async_copy(density, own.at[:, pl.ds(PAD, rows), :], local_sem.at[0])
    kind_load = pltpu.make_async_copy(kind, kinds, local_sem.at[1])

    own_load.start()
    kind_load.start()
    pl.semaphore_wait(barrier, devices - 1)
    for k in range(min(WINDOW, steps)):
        x_copy(k).start()
    own_halo.start()

    x_band[...] = band((cols, cols), 0)
    acc[...] = jnp.zeros_like(acc)
    along_z[:, pl.ds(edge, PAD), :] = jnp.zeros((depth, PAD, cols), jnp.float32)

    @pl.when(jnp.logical_not(has_source))
    def _():
        @pl.loop(0, RADIUS)
        def _(k):
            far[k] = jnp.zeros(far.shape[1:], jnp.float32)

    beta = beta_ref[0]

    def filter_z(start, count):
        for r in range(0, count, 8):
            for c in range(0, cols, LANES):
                at = (pl.ds(pl.multiple_of(start + r, 8), 8), pl.ds(c, LANES))
                values = [far[jnp.where(even, m, RADIUS - 1 - m), at[0], at[1]] for m in range(RADIUS)]
                values += [own[jnp.where(even, i, depth - 1 - i), at[0], at[1]] for i in range(depth)]
                values += [near[jnp.where(even, i, depth - 1 - i), at[0], at[1]] for i in range(RADIUS)]
                for i, out in enumerate(box(box(values))):
                    along_z[jnp.where(even, i, depth - 1 - i), at[0], at[1]] = out

    def filter_yx(j):
        r = row_of(j)
        y_band = band((CHUNK, CHUNK + 2 * PAD), PAD)
        pieces = []
        for layer in range(depth):
            high, low = split(along_z[layer, pl.ds(r, CHUNK + 2 * PAD), :])
            pieces.append(jnp.dot(y_band, high, preferred_element_type=jnp.float32)
                          + jnp.dot(y_band, low, preferred_element_type=jnp.float32))
        high, low = split(jnp.concatenate(pieces, axis=0))
        smoothed = (jnp.dot(high, x_band[...], preferred_element_type=jnp.float32)
                    + jnp.dot(low, x_band[...], preferred_element_type=jnp.float32))
        row = lax.broadcasted_iota(jnp.int32, (CHUNK, cols), 0) + (pencil * rows + r)
        col = lax.broadcasted_iota(jnp.int32, (CHUNK, cols), 1)
        cover_y = coverage(row, rows * pencils)
        cover_x = coverage(col, cols)
        for layer in range(depth):
            depth_index = jnp.full((1, cols), slab * depth + layer, jnp.int32)
            cover = coverage(depth_index, slabs * depth) * cover_y * cover_x
            filtered = smoothed[layer * CHUNK : (layer + 1) * CHUNK] / cover
            which = kinds[layer, pl.ds(r, CHUNK), :]
            value = jnp.where(which == 0, filtered, jnp.where(which == 2, FAR, -FAR))
            coded[layer, pl.ds(r, CHUNK), :] = value
            tangent = jnp.tanh(beta * (value - 0.5))
            acc[0] += folded(tangent)
            acc[1] += folded(1.0 - tangent * tangent)

    @pl.loop(0, steps + lag + 1)
    def _(k):
        @pl.when(k < steps)
        def _():
            x_copy(k).wait_recv()

            @pl.when(has_target)
            def _():
                f_copy(k).start()

        @pl.when(k + WINDOW < steps)
        def _():
            x_copy(k + WINDOW).start()

            @pl.when(k + WINDOW >= lead)
            def _():
                b_copy(k + WINDOW - lead).start()

        @pl.when(k + WINDOW == steps)
        def _():
            @pl.loop(max(steps - lead, 0), steps)
            def _(j):
                b_copy(j).start()

        @pl.when((k >= lag) & (k < steps + lag))
        def _():
            b_copy(k - lag).wait_recv()

            @pl.when(k == lag)
            def _():
                near_halo.start()

            @pl.when(has_source)
            def _():
                f_copy(k - lag).wait_recv()

                @pl.when(k == lag)
                def _():
                    far_halo.start()

            @pl.when(k == lag)
            def _():
                own_load.wait()
                kind_load.wait()

            filter_z(row_of(k - lag) + PAD, CHUNK)

        @pl.when(k == lag + 1)
        def _():
            own_halo.wait_recv()
            near_halo.wait_recv()

            @pl.when(has_source)
            def _():
                far_halo.wait_recv()

            filter_z(halo, PAD)

        @pl.when(k >= lag + 1)
        def _():
            filter_yx(k - lag - 1)

    cells = float(devices) * float(depth * rows * cols)
    level = jnp.full((1, 1), 0.5, jnp.float32)
    for step in range(ITERS):
        if step:
            center = jnp.broadcast_to(level, (8, cols))

            def body(i, carry):
                total, bend = carry
                for layer in range(depth):
                    tangent = jnp.tanh(beta * (coded[layer, pl.ds(pl.multiple_of(i * 8, 8), 8), :] - center))
                    total = total + tangent
                    bend = bend + (1.0 - tangent * tangent)
                return total, bend

            zero = jnp.zeros((8, cols), jnp.float32)
            total, bend = lax.fori_loop(0, rows // 8, body, (zero, zero))
            total, bend = folded(total), folded(bend)
        else:
            total, bend = acc[0], acc[1]
        parts[step, me] = jnp.concatenate(
            [jnp.sum(total, axis=0, keepdims=True), jnp.sum(bend, axis=0, keepdims=True)], axis=0)

        def send(there, core):
            pltpu.make_async_remote_copy(
                parts.at[step, me], parts.at[step, me], r_send.at[step], r_recv.at[step],
                device_id=(there, core), device_id_type=MESH).start()

        def send_all(k, carry):
            there = slab + (slabs - k)
            there = there - jnp.where(there >= slabs, slabs, 0)
            for core in range(pencils):
                send(there, core)
            return carry

        lax.fori_loop(1, slabs, send_all, 0, unroll=5 if slabs % 5 == 1 else 1)
        send(slab, sibling)

        most = parts.at[step, pl.ds(0, devices - 1)]
        pltpu.make_async_copy(most, most, r_recv.at[step]).wait()
        both = jnp.sum(jnp.sum(parts[step], axis=0), axis=1, keepdims=True)
        volume = 0.5 * (cells + both[0:1])
        slope = cells + 0.5 * beta * both[1:2]
        level = level + (volume - fraction_ref[0] * cells) / slope
    level_out[...] = jnp.broadcast_to(level, level_out.shape)

    @pl.loop(0, steps)
    def _(k):
        x_copy(k).wait_send()
        b_copy(k).wait_send()

        @pl.when(has_target)
        def _():
            f_copy(k).wait_send()

    own_halo.wait_send()
    near_halo.wait_send()

    @pl.when(has_source)
    def _():
        far_halo.wait_send()

    for step in range(ITERS):
        most = parts.at[step, pl.ds(0, devices - 1)]
        pltpu.make_async_copy(most, most, r_send.at[step]).wait()


def solution(mesh):
    slabs, pencils = mesh.shape["slab"], mesh.shape["pencil"]

    def local(density, cell_kind, sharpness, fraction):
        depth, rows, cols = density.shape
        steps = rows // CHUNK
        wide = rows + 2 * PAD
        coded, level = pl.pallas_call(
            functools.partial(kernel, slabs, pencils),
            out_shape=(jax.ShapeDtypeStruct(density.shape, jnp.float32), jax.ShapeDtypeStruct((1, LANES), jnp.float32)),
            in_specs=[pl.BlockSpec(memory_space=pltpu.SMEM)] * 2 + [pl.BlockSpec(memory_space=pltpu.HBM)] * 2,
            out_specs=(pl.BlockSpec(memory_space=pltpu.VMEM), pl.BlockSpec(memory_space=pltpu.VMEM)),
            scratch_shapes=[
                pltpu.VMEM((depth, wide, cols), jnp.float32),
                pltpu.VMEM((depth, wide, cols), jnp.float32),
                pltpu.VMEM((RADIUS, wide, cols), jnp.float32),
                pltpu.VMEM((depth, rows, cols), jnp.int32),
                pltpu.VMEM((depth, wide, cols), jnp.float32),
                pltpu.VMEM((cols, cols), jnp.bfloat16),
                pltpu.VMEM((2, 8, LANES), jnp.float32),
                pltpu.VMEM((ITERS, slabs * pencils, 2, LANES), jnp.float32),
                pltpu.SemaphoreType.DMA((steps,)),
                pltpu.SemaphoreType.DMA((steps,)),
                pltpu.SemaphoreType.DMA((steps,)),
                pltpu.SemaphoreType.DMA((steps,)),
                pltpu.SemaphoreType.DMA((steps,)),
                pltpu.SemaphoreType.DMA((steps,)),
                pltpu.SemaphoreType.DMA((3,)),
                pltpu.SemaphoreType.DMA((3,)),
                pltpu.SemaphoreType.DMA((2,)),
                pltpu.SemaphoreType.DMA((ITERS,)),
                pltpu.SemaphoreType.DMA((ITERS,)),
            ],
            compiler_params=pltpu.CompilerParams(
                collective_id=0, has_side_effects=True, vmem_limit_bytes=49 * 1024 * 1024),
        )(sharpness, fraction, density, cell_kind)
        threshold = level[0, :1]
        physical = 0.5 * (1.0 + jnp.tanh(sharpness[0] * (coded - threshold[0])))
        return physical, threshold

    in_specs = (P("slab", "pencil", None), P("slab", "pencil", None), P(), P())
    out_specs = (P("slab", "pencil", None), P())
    return jax.shard_map(local, mesh=mesh, in_specs=in_specs, out_specs=out_specs, check_vma=False)
```

```python
import functools

import jax
import jax.numpy as jnp
from jax import lax
from jax.experimental import pallas as pl
from jax.experimental.pallas import tpu as pltpu
from jax.sharding import PartitionSpec as P

RADIUS = 5
ITERS = 3
CHUNK = 16
PAD = 8
WINDOW = 4
LEAD = 8
LANES = 128
FAR = 1.0e6
MESH = pl.DeviceIdType.MESH


def box(values):
    pairs = [a + b for a, b in zip(values[:-1], values[1:])]
    return [pairs[k] + pairs[k + 2] + pairs[k + 4] for k in range(len(values) - RADIUS)]


def triangle(k):
    k = jnp.maximum(k, 0)
    return (k * (k + 1)) // 2


def coverage(index, whole):
    full = (RADIUS + 1) * (RADIUS + 1)
    return (full - triangle(RADIUS - index) - triangle(RADIUS + 1 + index - whole)).astype(jnp.float32)


def split(x):
    high = x.astype(jnp.bfloat16)
    return high, (x - high.astype(jnp.float32)).astype(jnp.bfloat16)


def band(shape, shift):
    row = lax.broadcasted_iota(jnp.int32, shape, 0)
    col = lax.broadcasted_iota(jnp.int32, shape, 1)
    return jnp.maximum(RADIUS + 1 - jnp.abs(col - shift - row), 0).astype(jnp.float32).astype(jnp.bfloat16)


def folded(x):
    tiles = [
        x[i : i + 8, j : j + LANES] for i in range(0, x.shape[0], 8) for j in range(0, x.shape[1], LANES)
    ]
    while len(tiles) > 1:
        tiles = [sum(tiles[i : i + 2][1:], tiles[i]) for i in range(0, len(tiles), 2)]
    return tiles[0]


def kernel(slabs, pencils, beta_ref, fraction_ref, density, kind, coded, level_out, own, near, far, kinds,
           along_z, x_band, acc, parts, x_send, x_recv, b_send, b_recv, f_send, f_recv, h_send, h_recv, local_sem,
           r_send, r_recv):
    depth, rows, cols = density.shape
    steps = rows // CHUNK
    lead = min(LEAD, steps)
    lag = lead + 1
    slab = lax.axis_index("slab")
    pencil = lax.axis_index("pencil")
    even = slab % 2 == 0
    first = pencil == 0
    devices = slabs * pencils
    me = slab * pencils + pencil

    barrier = pltpu.get_barrier_semaphore()

    def greet(k, carry):
        there = slab + (slabs - k)
        there = there - jnp.where(there >= slabs, slabs, 0)
        for core in range(pencils):
            pl.semaphore_signal(barrier, inc=1, device_id=(there, core), device_id_type=MESH)
        return carry

    lax.fori_loop(1, slabs, greet, 0, unroll=15 if slabs % 15 == 1 else 1)
    pl.semaphore_signal(barrier, inc=1, device_id=(slab, 1 - pencil), device_id_type=MESH)

    partner = slab + jnp.where(even, 1, -1)
    target = slab + jnp.where(even, 2, -2)
    source = slab - jnp.where(even, 2, -2)
    has_target = (target >= 0) & (target < slabs)
    has_source = (source >= 0) & (source < slabs)
    target = jnp.clip(target, 0, slabs - 1)
    sibling = 1 - pencil
    halo = pl.multiple_of(jnp.where(first, PAD + rows, 0), 8)
    edge = pl.multiple_of(jnp.where(first, 0, PAD + rows), 8)
    there = pl.multiple_of(jnp.where(first, 0, PAD + rows), 8)
    mine = pl.multiple_of(jnp.where(first, rows, PAD), 8)

    def row_of(k):
        return pl.multiple_of(jnp.where(first, steps - 1 - k, k) * CHUNK, CHUNK)

    def x_copy(k):
        r = row_of(k)
        layers = pl.ds(jnp.where(even, 0, depth - RADIUS), RADIUS)
        return pltpu.make_async_remote_copy(
            density.at[layers, pl.ds(r, CHUNK), :], near.at[layers, pl.ds(r + PAD, CHUNK), :],
            x_send.at[k], x_recv.at[k], device_id=(partner, pencil), device_id_type=MESH)

    def b_copy(k):
        r = row_of(k)
        layers = pl.ds(jnp.where(even, RADIUS, 0), depth - RADIUS)
        return pltpu.make_async_remote_copy(
            density.at[layers, pl.ds(r, CHUNK), :], near.at[layers, pl.ds(r + PAD, CHUNK), :],
            b_send.at[k], b_recv.at[k], device_id=(partner, pencil), device_id_type=MESH)

    def f_copy(k):
        r = row_of(k)
        start = jnp.where(even, depth - RADIUS, 0)
        return pltpu.make_async_remote_copy(
            near.at[pl.ds(start, RADIUS), pl.ds(r + PAD, CHUNK), :], far.at[:, pl.ds(r + PAD, CHUNK), :],
            f_send.at[k], f_recv.at[k], device_id=(target, pencil), device_id_type=MESH)

    def halo_copy(index, src, dst):
        return pltpu.make_async_remote_copy(
            src, dst, h_send.at[index], h_recv.at[index], device_id=(slab, sibling), device_id_type=MESH)

    own_row = pl.multiple_of(jnp.where(first, rows - PAD, 0), 8)
    own_halo = halo_copy(0, density.at[:, pl.ds(own_row, PAD), :], own.at[:, pl.ds(there, PAD), :])
    near_halo = halo_copy(1, near.at[:, pl.ds(mine, PAD), :], near.at[:, pl.ds(there, PAD), :])
    far_halo = halo_copy(2, far.at[:, pl.ds(mine, PAD), :], far.at[:, pl.ds(there, PAD), :])
    own_load = pltpu.make_async_copy(density, own.at[:, pl.ds(PAD, rows), :], local_sem.at[0])
    kind_load = pltpu.make_async_copy(kind, kinds, local_sem.at[1])

    own_load.start()
    kind_load.start()
    pl.semaphore_wait(barrier, devices - 1)
    for k in range(min(WINDOW, steps)):
        x_copy(k).start()
    own_halo.start()

    x_band[...] = band((cols, cols), 0)
    acc[...] = jnp.zeros_like(acc)
    along_z[:, pl.ds(edge, PAD), :] = jnp.zeros((depth, PAD, cols), jnp.float32)

    @pl.when(jnp.logical_not(has_source))
    def _():
        @pl.loop(0, RADIUS)
        def _(k):
            far[k] = jnp.zeros(far.shape[1:], jnp.float32)

    beta = beta_ref[0]

    def filter_z(start, count):
        for r in range(0, count, 8):
            for c in range(0, cols, LANES):
                at = (pl.ds(pl.multiple_of(start + r, 8), 8), pl.ds(c, LANES))
                values = [far[jnp.where(even, m, RADIUS - 1 - m), at[0], at[1]] for m in range(RADIUS)]
                values += [own[jnp.where(even, i, depth - 1 - i), at[0], at[1]] for i in range(depth)]
                values += [near[jnp.where(even, i, depth - 1 - i), at[0], at[1]] for i in range(RADIUS)]
                for i, out in enumerate(box(box(values))):
                    along_z[jnp.where(even, i, depth - 1 - i), at[0], at[1]] = out

    def filter_yx(j):
        r = row_of(j)
        y_band = band((CHUNK, CHUNK + 2 * PAD), PAD)
        pieces = []
        for layer in range(depth):
            high, low = split(along_z[layer, pl.ds(r, CHUNK + 2 * PAD), :])
            pieces.append(jnp.dot(y_band, high, preferred_element_type=jnp.float32)
                          + jnp.dot(y_band, low, preferred_element_type=jnp.float32))
        high, low = split(jnp.concatenate(pieces, axis=0))
        smoothed = (jnp.dot(high, x_band[...], preferred_element_type=jnp.float32)
                    + jnp.dot(low, x_band[...], preferred_element_type=jnp.float32))
        row = lax.broadcasted_iota(jnp.int32, (CHUNK, cols), 0) + (pencil * rows + r)
        col = lax.broadcasted_iota(jnp.int32, (CHUNK, cols), 1)
        cover_y = coverage(row, rows * pencils)
        cover_x = coverage(col, cols)
        for layer in range(depth):
            depth_index = jnp.full((1, cols), slab * depth + layer, jnp.int32)
            cover = coverage(depth_index, slabs * depth) * cover_y * cover_x
            filtered = smoothed[layer * CHUNK : (layer + 1) * CHUNK] / cover
            which = kinds[layer, pl.ds(r, CHUNK), :]
            value = jnp.where(which == 0, filtered, jnp.where(which == 2, FAR, -FAR))
            coded[layer, pl.ds(r, CHUNK), :] = value
            tangent = jnp.tanh(beta * (value - 0.5))
            acc[0] += folded(tangent)
            acc[1] += folded(1.0 - tangent * tangent)

    @pl.loop(0, steps + lag + 1)
    def _(k):
        @pl.when(k < steps)
        def _():
            x_copy(k).wait_recv()

            @pl.when(has_target)
            def _():
                f_copy(k).start()

        @pl.when(k + WINDOW < steps)
        def _():
            x_copy(k + WINDOW).start()

            @pl.when(k + WINDOW >= lead)
            def _():
                b_copy(k + WINDOW - lead).start()

        @pl.when(k + WINDOW == steps)
        def _():
            @pl.loop(max(steps - lead, 0), steps)
            def _(j):
                b_copy(j).start()

        @pl.when((k >= lag) & (k < steps + lag))
        def _():
            b_copy(k - lag).wait_recv()

            @pl.when(k == lag)
            def _():
                near_halo.start()

            @pl.when(has_source)
            def _():
                f_copy(k - lag).wait_recv()

                @pl.when(k == lag)
                def _():
                    far_halo.start()

            @pl.when(k == lag)
            def _():
                own_load.wait()
                kind_load.wait()

            filter_z(row_of(k - lag) + PAD, CHUNK)

        @pl.when(k == lag + 1)
        def _():
            own_halo.wait_recv()
            near_halo.wait_recv()

            @pl.when(has_source)
            def _():
                far_halo.wait_recv()

            filter_z(halo, PAD)

        @pl.when(k >= lag + 1)
        def _():
            filter_yx(k - lag - 1)

    cells = float(devices) * float(depth * rows * cols)
    level = jnp.full((1, 1), 0.5, jnp.float32)
    for step in range(ITERS):
        if step:
            center = jnp.broadcast_to(level, (8, cols))

            def body(i, carry):
                total, bend = carry
                for layer in range(depth):
                    tangent = jnp.tanh(beta * (coded[layer, pl.ds(pl.multiple_of(i * 8, 8), 8), :] - center))
                    total = total + tangent
                    bend = bend + (1.0 - tangent * tangent)
                return total, bend

            zero = jnp.zeros((8, cols), jnp.float32)
            total, bend = lax.fori_loop(0, rows // 8, body, (zero, zero), unroll=2)
            total, bend = folded(total), folded(bend)
        else:
            total, bend = acc[0], acc[1]
        parts[step, me] = jnp.concatenate(
            [jnp.sum(total, axis=0, keepdims=True), jnp.sum(bend, axis=0, keepdims=True)], axis=0)

        def send(there, core):
            pltpu.make_async_remote_copy(
                parts.at[step, me], parts.at[step, me], r_send.at[step], r_recv.at[step],
                device_id=(there, core), device_id_type=MESH).start()

        def send_all(k, carry):
            there = slab + (slabs - k)
            there = there - jnp.where(there >= slabs, slabs, 0)
            for core in range(pencils):
                send(there, core)
            return carry

        lax.fori_loop(1, slabs, send_all, 0, unroll=15 if slabs % 15 == 1 else 1)
        send(slab, sibling)

        most = parts.at[step, pl.ds(0, devices - 1)]
        pltpu.make_async_copy(most, most, r_recv.at[step]).wait()
        both = jnp.sum(jnp.sum(parts[step], axis=0), axis=1, keepdims=True)
        volume = 0.5 * (cells + both[0:1])
        slope = cells + 0.5 * beta * both[1:2]
        level = level + (volume - fraction_ref[0] * cells) / slope
    level_out[...] = jnp.broadcast_to(level, level_out.shape)

    @pl.loop(0, steps)
    def _(k):
        x_copy(k).wait_send()
        b_copy(k).wait_send()

        @pl.when(has_target)
        def _():
            f_copy(k).wait_send()

    own_halo.wait_send()
    near_halo.wait_send()

    @pl.when(has_source)
    def _():
        far_halo.wait_send()

    for step in range(ITERS):
        most = parts.at[step, pl.ds(0, devices - 1)]
        pltpu.make_async_copy(most, most, r_send.at[step]).wait()


def solution(mesh):
    slabs, pencils = mesh.shape["slab"], mesh.shape["pencil"]

    def local(density, cell_kind, sharpness, fraction):
        depth, rows, cols = density.shape
        steps = rows // CHUNK
        wide = rows + 2 * PAD
        coded, level = pl.pallas_call(
            functools.partial(kernel, slabs, pencils),
            out_shape=(jax.ShapeDtypeStruct(density.shape, jnp.float32), jax.ShapeDtypeStruct((1, LANES), jnp.float32)),
            in_specs=[pl.BlockSpec(memory_space=pltpu.SMEM)] * 2 + [pl.BlockSpec(memory_space=pltpu.HBM)] * 2,
            out_specs=(pl.BlockSpec(memory_space=pltpu.VMEM), pl.BlockSpec(memory_space=pltpu.VMEM)),
            scratch_shapes=[
                pltpu.VMEM((depth, wide, cols), jnp.float32),
                pltpu.VMEM((depth, wide, cols), jnp.float32),
                pltpu.VMEM((RADIUS, wide, cols), jnp.float32),
                pltpu.VMEM((depth, rows, cols), jnp.int32),
                pltpu.VMEM((depth, wide, cols), jnp.float32),
                pltpu.VMEM((cols, cols), jnp.bfloat16),
                pltpu.VMEM((2, 8, LANES), jnp.float32),
                pltpu.VMEM((ITERS, slabs * pencils, 2, LANES), jnp.float32),
                pltpu.SemaphoreType.DMA((steps,)),
                pltpu.SemaphoreType.DMA((steps,)),
                pltpu.SemaphoreType.DMA((steps,)),
                pltpu.SemaphoreType.DMA((steps,)),
                pltpu.SemaphoreType.DMA((steps,)),
                pltpu.SemaphoreType.DMA((steps,)),
                pltpu.SemaphoreType.DMA((3,)),
                pltpu.SemaphoreType.DMA((3,)),
                pltpu.SemaphoreType.DMA((2,)),
                pltpu.SemaphoreType.DMA((ITERS,)),
                pltpu.SemaphoreType.DMA((ITERS,)),
            ],
            compiler_params=pltpu.CompilerParams(
                collective_id=0, has_side_effects=True, vmem_limit_bytes=49 * 1024 * 1024),
        )(sharpness, fraction, density, cell_kind)
        threshold = level[0, :1]
        physical = 0.5 * (1.0 + jnp.tanh(sharpness[0] * (coded - threshold[0])))
        return physical, threshold

    in_specs = (P("slab", "pencil", None), P("slab", "pencil", None), P(), P())
    out_specs = (P("slab", "pencil", None), P())
    return jax.shard_map(local, mesh=mesh, in_specs=in_specs, out_specs=out_specs, check_vma=False)
```
